32 devices in a mesh: seq: 8 (over z, x), feat: 4 (over y, core).
Axes of the slice: x: 2, y: 2, z: 4, core: 2. Of those that a mesh axis runs over, the one named last changes fastest.
Arguments:
- injection: bfloat16 [1024, 5120], P('seq', 'feat'), may hold values from -8 to 8
- warm_start: bfloat16 [1024, 5120], P('seq', 'feat'), may hold values from -12 to 12
- gain_in: float32 [5120], replicated, may hold values from 0.5 to 1.5
- gain_out: float32 [5120], replicated, may hold values from 0.5 to 1.5
- w_query: bfloat16 [5120, 5120], P(None, 'feat'), may hold values from -0.0848993624 to 0.0848993624
- w_key: bfloat16 [5120, 1024], P(None, 'feat'), may hold values from -0.0848993624 to 0.0848993624
- w_value: bfloat16 [5120, 1024], P(None, 'feat'), may hold values from -0.078125 to 0.078125
- w_out: bfloat16 [5120, 5120], P('feat'), may hold values from -0.078125 to 0.078125
Outputs:
- equilibrium: float32 [1024, 5120], P('seq', 'feat')
The draws below stay inside these ranges and needn't reach their ends.
All inputs are finite; a program needn't handle non-finite values.
Results may differ from the reference program's by a relative error of at most 0.009.
Values may be sent and summed in bfloat16 or wider, within the bound.
A program may use at most 128 MiB of HBM per device.

```python
import math
import jax
import jax.numpy as jnp
from jax import lax

D = 5120
HEADS = 40
KV_HEADS = 8
HEAD_DIM = 128
ITERS = 4
TOKENS = 1024


ALIGN_TARGET = 325.0


def align_scale():
    return math.sqrt(ALIGN_TARGET / (D * math.sqrt(HEAD_DIM)))


def spike_layout(key):
    sign_query = jax.random.randint(jax.random.fold_in(key, 7001), (D,), 0, 2).astype(jnp.float32) * 2.0 - 1.0
    sign_key = jax.random.randint(jax.random.fold_in(key, 7002), (D,), 0, 2).astype(jnp.float32) * 2.0 - 1.0
    half_tokens = TOKENS // 2
    key_places = jax.random.permutation(jax.random.fold_in(key, 7003), half_tokens)[:8].astype(jnp.int32)
    query_places = (jax.random.permutation(jax.random.fold_in(key, 7004), half_tokens)[:8] + half_tokens).astype(jnp.int32)
    return (sign_query, sign_key, key_places, query_places)


def matrix_noise(key, columns):
    noise_part = jnp.clip(jax.random.normal(key, (D, columns), jnp.float32), -6.0, 6.0)
    return noise_part / math.sqrt(D)


def draw_injection(key, part):
    sign_query, sign_key, key_places, query_places = spike_layout(key)
    base_noise = jnp.clip(jax.random.normal(jax.random.fold_in(key, 11), (TOKENS, D), jnp.float32), -4.0, 4.0)
    position = jnp.arange(TOKENS, dtype=jnp.int32)
    query_strength = jnp.array([0.5, 0.5, 1.0, 1.0, 2.0, 2.0, 4.0, 4.0], jnp.float32)
    query_weight = jnp.sum(jnp.where(position[None, :] == query_places[:, None], query_strength[:, None], 0.0), axis=0)
    key_weight = jnp.sum(jnp.where(position[None, :] == key_places[:, None], 3.0, 0.0), axis=0)
    result = base_noise + query_weight[:, None] * sign_query[None, :] + key_weight[:, None] * sign_key[None, :]
    return result.astype(jnp.bfloat16)


def draw_w_query(key, part):
    sign_query, sign_key, key_places, query_places = spike_layout(key)
    noise_part = matrix_noise(jax.random.fold_in(key, 21), HEADS * HEAD_DIM)
    result = noise_part + align_scale() * sign_query[:, None] / math.sqrt(D)
    return result.astype(jnp.bfloat16)


def draw_w_key(key, part):
    sign_query, sign_key, key_places, query_places = spike_layout(key)
    noise_part = matrix_noise(jax.random.fold_in(key, 22), KV_HEADS * HEAD_DIM)
    result = noise_part + align_scale() * sign_key[:, None] / math.sqrt(D)
    return result.astype(jnp.bfloat16)


def draw_warm_start(key, part):
    row_frac = jnp.arange(TOKENS, dtype=jnp.float32) / (TOKENS - 1)
    col_frac = jnp.arange(D, dtype=jnp.float32) / (D - 1)
    row_rough = jnp.exp(jax.random.uniform(jax.random.fold_in(key, 31), (TOKENS,), jnp.float32, math.log(0.7), math.log(1.4)))
    col_rough = jnp.exp(jax.random.uniform(jax.random.fold_in(key, 32), (D,), jnp.float32, math.log(0.7), math.log(1.4)))
    col_scale = (0.6 + 0.9 * col_frac) * col_rough
    base_noise = jnp.clip(jax.random.normal(jax.random.fold_in(key, 33), (TOKENS, D), jnp.float32), -4.0, 4.0)
    row_scale = jnp.exp(math.log(0.25) + row_frac * math.log(10.0)) * row_rough
    result = base_noise * row_scale[:, None] * col_scale[None, :]
    return jnp.clip(result, -12.0, 12.0).astype(jnp.bfloat16)


def shard_levels(stream_key, shape, cuts, smallest, largest):
    loudness, own = 1.0, jax.random.fold_in(stream_key, 6)
    for dim, parts in cuts:
        heights = jnp.exp(jax.random.uniform(jax.random.fold_in(own, dim), (parts,), jnp.float32, smallest / len(cuts), largest / len(cuts)))
        loudness = loudness * jnp.repeat(heights, shape[dim] // parts).reshape([-1 if axis == dim else 1 for axis in range(len(shape))])
    return loudness


def centred(own_key, dims, width, limit, pieces=(), kind=jnp.bfloat16):
    values = jax.random.normal(own_key, dims, jnp.float32) * width
    if len(pieces) > 0:
        values = shard_levels(own_key, dims, pieces, -0.22, 0.18) * values
    return jnp.clip(values, min=-limit, max=limit).astype(kind)


def setup_inputs(seed: int = 0) -> dict:
    splits = jax.random.split(jax.random.key(seed), 9)
    return {
        "injection": draw_injection(jax.random.fold_in(splits[8], 71), 0),
        "warm_start": draw_warm_start(jax.random.fold_in(splits[8], 71), 0),
        "gain_in": jnp.clip(1.0 + 0.1 * jax.random.normal(splits[2], (D,), jnp.float32), 0.5, 1.5),
        "gain_out": jnp.clip(1.0 + 0.1 * jax.random.normal(splits[3], (D,), jnp.float32), 0.5, 1.5),
        "w_query": draw_w_query(jax.random.fold_in(splits[8], 71), 0),
        "w_key": draw_w_key(jax.random.fold_in(splits[8], 71), 0),
        "w_value": centred(splits[6], (D, KV_HEADS * HEAD_DIM), D ** -0.5, 0.078125, ((1, 4),)),
        "w_out": centred(splits[7], (HEADS * HEAD_DIM, D), (HEADS * HEAD_DIM) ** -0.5, 0.078125, ((0, 4),)),
    }


EPS = 1e-06
LAMBDA = 0.03

def rms_scale(matrix, gain_vec):
    return matrix * lax.rsqrt(lax.optimization_barrier(jnp.mean(matrix * matrix, axis=-1, keepdims=True)) + EPS) * gain_vec

def solve_small(matrix, target):
    size_now = target.shape[0]
    row_list = [matrix[idx_row] for idx_row in range(size_now)]
    value_list = [target[idx_row] for idx_row in range(size_now)]
    for pivot_at in range(size_now):
        for below_at in range(pivot_at + 1, size_now):
            ratio_now = row_list[below_at][pivot_at] / row_list[pivot_at][pivot_at]
            row_list[below_at] = row_list[below_at] - ratio_now * row_list[pivot_at]
            value_list[below_at] = value_list[below_at] - ratio_now * value_list[pivot_at]
    result_list = [None] * size_now
    for pivot_at in reversed(range(size_now)):
        running = value_list[pivot_at]
        for later_at in range(pivot_at + 1, size_now):
            running = running - row_list[pivot_at][later_at] * result_list[later_at]
        result_list[pivot_at] = running / row_list[pivot_at][pivot_at]
    return jnp.stack(result_list)

def coefficients(gram_matrix):
    history_len = gram_matrix.shape[0]
    system = gram_matrix / (TOKENS * D) + LAMBDA * jnp.eye(history_len, dtype=jnp.float32)
    unscaled = solve_small(system, jnp.ones((history_len,), jnp.float32))
    return unscaled / jnp.sum(unscaled)

def layer(current, injection, gain_in, gain_out, w_query, w_key, w_value, w_out):
    group = HEADS // KV_HEADS
    mixed = current + injection.astype(jnp.float32)
    normed = rms_scale(mixed, gain_in).astype(jnp.bfloat16)
    queries = jnp.dot(normed, w_query, preferred_element_type=jnp.float32).astype(jnp.bfloat16)
    key_rows = jnp.dot(normed, w_key, preferred_element_type=jnp.float32).astype(jnp.bfloat16)
    value_rows = jnp.dot(normed, w_value, preferred_element_type=jnp.float32).astype(jnp.bfloat16)
    queries = queries.reshape(TOKENS, KV_HEADS, group, HEAD_DIM).transpose(1, 2, 0, 3)
    key_rows = key_rows.reshape(TOKENS, KV_HEADS, HEAD_DIM).transpose(1, 0, 2)
    value_rows = value_rows.reshape(TOKENS, KV_HEADS, HEAD_DIM).transpose(1, 0, 2)
    position = jnp.arange(TOKENS, dtype=jnp.int32)
    allowed = position[:, None] >= position[None, :]
    score_scale = 1.0 / math.sqrt(HEAD_DIM)

    def one_head(operands):
        query_head, key_head, value_head = operands
        scores = jnp.einsum('gtd,sd->gts', query_head.astype(jnp.float32), key_head.astype(jnp.float32)) * score_scale
        scores = jnp.where(allowed[None], scores, -1e+30)
        row_max = lax.optimization_barrier(jnp.max(scores, axis=-1, keepdims=True))
        weights = jnp.where(allowed[None], jnp.exp(scores - row_max), 0.0)
        row_sum = lax.optimization_barrier(jnp.sum(weights, axis=-1, keepdims=True))
        summed = jnp.einsum('gts,sd->gtd', weights.astype(jnp.bfloat16).astype(jnp.float32), value_head.astype(jnp.float32))
        return (summed / row_sum).astype(jnp.bfloat16)
    attended = lax.map(one_head, (queries, key_rows, value_rows))
    attended = attended.transpose(2, 0, 1, 3).reshape(TOKENS, HEADS * HEAD_DIM)
    update = jnp.dot(attended, w_out, preferred_element_type=jnp.float32)
    return rms_scale(mixed + update, gain_out)

def reference(injection, warm_start, gain_in, gain_out, w_query, w_key, w_value, w_out):
    params = (injection, gain_in, gain_out, w_query, w_key, w_value, w_out)
    current = warm_start.astype(jnp.float32)
    evaluated = []
    residuals = []
    for iteration in range(ITERS):
        image = layer(current, *params)
        evaluated.append(image)
        residuals.append(image - current)
        if iteration == 0:
            current = image
        else:
            history_len = iteration + 1
            gram_matrix = jnp.stack([jnp.stack([jnp.sum(residuals[row_at] * residuals[col_at]) for col_at in range(history_len)]) for row_at in range(history_len)])
            weights_now = coefficients(gram_matrix)
            current = weights_now[0] * evaluated[0]
            for other in range(1, history_len):
                current = current + weights_now[other] * evaluated[other]
    return current
```

```python
import functools
import math

import jax
import jax.numpy as jnp
from jax import lax
from jax.experimental import pallas as pl
from jax.experimental.pallas import tpu as pltpu
from jax.sharding import PartitionSpec as P

HEADS = 40
KV_HEADS = 8
HEAD_DIM = 128
ITERS = 4

EPS = 1e-06
LAMBDA = 0.03
MESH = pl.DeviceIdType.MESH
VMEM = pl.BlockSpec(memory_space=pltpu.VMEM)


def greet(axis, peers):
    barrier = pltpu.get_barrier_semaphore()
    for peer in peers:
        pl.semaphore_signal(barrier, inc=1, device_id={axis: peer}, device_id_type=MESH)
    return barrier


def send(src, dst, send_sem, recv_sem, axis, target):
    copy = pltpu.make_async_remote_copy(
        src_ref=src, dst_ref=dst, send_sem=send_sem, recv_sem=recv_sem,
        device_id={axis: target}, device_id_type=MESH,
    )
    copy.start()
    return copy


def place(axis, n):
    me = lax.axis_index(axis)
    side = lax.rem(me, 2)
    mine = lax.div(me, 2)
    return me, side, mine, me + 1 - 2 * side, n // 2


def gather_kernel(axis, n, chunks, x_ref, o_ref, send_sem, recv_sem, own_sem):
    me, side, mine, partner, lines = place(axis, n)
    rows = x_ref.shape[0] // chunks
    peers = [2 * lax.rem(mine + d, lines) + side for d in range(1, lines)]
    barrier = greet(axis, [partner] + peers)
    own = pltpu.make_async_copy(x_ref, o_ref.at[me], own_sem)
    own.start()
    pl.semaphore_wait(barrier, lines)
    pending = []
    arrivals = []
    for c in range(chunks):
        part = pl.ds(c * rows, rows)
        for d in range(1, lines):
            copy = send(x_ref.at[part], o_ref.at[me, part], send_sem.at[c, d], recv_sem.at[c, d], axis, peers[d - 1])
            arrivals.append((c, d, copy))
    for c in range(chunks):
        part = pl.ds(c * rows, rows)
        pending.append(
            send(x_ref.at[part], o_ref.at[me, part], send_sem.at[c, 0], recv_sem.at[c, 0], axis, partner)
        )
    for c, d, copy in arrivals:
        copy.wait_recv()
        part = pl.ds(c * rows, rows)
        source = 2 * lax.rem(mine - d + lines, lines) + side
        here = o_ref.at[source, part]
        at = lines - 1 + d
        pending.append(send(here, here, send_sem.at[c, at], recv_sem.at[c, at], axis, partner))
    for c, d, copy in arrivals:
        copy.wait_send()
    for copy in pending:
        copy.wait()
    own.wait()


def gather(x, axis, chunks, collective_id):
    n = lax.axis_size(axis)
    return pl.pallas_call(
        functools.partial(gather_kernel, axis, n, chunks),
        out_shape=jax.ShapeDtypeStruct((n,) + x.shape, x.dtype),
        in_specs=[VMEM],
        out_specs=VMEM,
        scratch_shapes=[
            pltpu.SemaphoreType.DMA((chunks, n)),
            pltpu.SemaphoreType.DMA((chunks, n)),
            pltpu.SemaphoreType.DMA,
        ],
        compiler_params=pltpu.CompilerParams(collective_id=collective_id, has_side_effects=True),
    )(x)


def scatter_kernel(axis, n, chunks, x_ref, o_ref, near, outgoing, far, near_s, near_r, far_s, far_r):
    me, side, mine, partner, lines = place(axis, n)
    rows = x_ref.shape[1] // chunks
    lined = [lax.rem(mine + d, lines) for d in range(lines)]
    barrier = greet(axis, [partner] + [2 * line + side for line in lined[1:]])
    pl.semaphore_wait(barrier, lines)
    nears = {}
    for c in range(chunks):
        part = pl.ds(c * rows, rows)
        for d in range(1, lines):
            nears[c, d] = send(
                x_ref.at[2 * lined[d] + 1 - side, part], near.at[d, part],
                near_s.at[c, d], near_r.at[c, d], axis, partner,
            )
    for c in range(chunks):
        part = pl.ds(c * rows, rows)
        nears[c, 0] = send(
            x_ref.at[partner, part], near.at[0, part], near_s.at[c, 0], near_r.at[c, 0], axis, partner
        )
    fars = {}
    for c in range(chunks):
        part = pl.ds(c * rows, rows)
        for d in range(1, lines):
            nears[c, d].wait_recv()
            outgoing[d, part] = (
                x_ref[2 * lined[d] + side, part].astype(jnp.float32) + near[d, part].astype(jnp.float32)
            ).astype(jnp.bfloat16)
            fars[c, d] = send(
                outgoing.at[d, part], far.at[d, part], far_s.at[c, d], far_r.at[c, d], axis,
                2 * lined[d] + side,
            )
    for c in range(chunks):
        part = pl.ds(c * rows, rows)
        nears[c, 0].wait_recv()
        total = x_ref[me, part].astype(jnp.float32) + near[0, part].astype(jnp.float32)
        for d in range(1, lines):
            fars[c, d].wait_recv()
            total = total + far[d, part].astype(jnp.float32)
        o_ref[part] = total
    for copy in list(nears.values()) + list(fars.values()):
        copy.wait_send()


def scatter(x, axis, chunks, collective_id):
    n = lax.axis_size(axis)
    lines = n // 2
    buffer = pltpu.VMEM((lines,) + x.shape[1:], x.dtype)
    return pl.pallas_call(
        functools.partial(scatter_kernel, axis, n, chunks),
        out_shape=jax.ShapeDtypeStruct(x.shape[1:], jnp.float32),
        in_specs=[VMEM],
        out_specs=VMEM,
        scratch_shapes=[buffer] * 3 + [pltpu.SemaphoreType.DMA((chunks, lines))] * 4,
        compiler_params=pltpu.CompilerParams(collective_id=collective_id, has_side_effects=True),
    )(x)


def exchange_kernel(axis, n, x_ref, o_ref, send_sem, recv_sem, own_sem):
    me = lax.axis_index(axis)
    peers = [lax.rem(me + d, n) for d in range(1, n)]
    barrier = greet(axis, peers)
    own = pltpu.make_async_copy(x_ref.at[me], o_ref.at[me], own_sem)
    own.start()
    pl.semaphore_wait(barrier, n - 1)
    copies = [
        send(x_ref.at[peer], o_ref.at[me], send_sem.at[d], recv_sem.at[d], axis, peer)
        for d, peer in enumerate(peers)
    ]
    for copy in copies:
        copy.wait()
    own.wait()


def exchange(x, axis, collective_id):
    n = lax.axis_size(axis)
    return pl.pallas_call(
        functools.partial(exchange_kernel, axis, n),
        out_shape=jax.ShapeDtypeStruct(x.shape, x.dtype),
        in_specs=[VMEM],
        out_specs=VMEM,
        scratch_shapes=[
            pltpu.SemaphoreType.DMA((n,)),
            pltpu.SemaphoreType.DMA((n,)),
            pltpu.SemaphoreType.DMA,
        ],
        compiler_params=pltpu.CompilerParams(collective_id=collective_id, has_side_effects=True),
    )(x)


def solve_values(rows, values):
    size = len(values)
    rows = [list(row) for row in rows]
    values = list(values)
    for pivot in range(size):
        for below in range(pivot + 1, size):
            ratio = rows[below][pivot] / rows[pivot][pivot]
            for at in range(pivot, size):
                rows[below][at] = rows[below][at] - ratio * rows[pivot][at]
            values[below] = values[below] - ratio * values[pivot]
    result = [None] * size
    for pivot in reversed(range(size)):
        running = values[pivot]
        for later in range(pivot + 1, size):
            running = running - rows[pivot][later] * result[later]
        result[pivot] = running / rows[pivot][pivot]
    return result


def new_products(count):
    return [(i, j) for i in range(count) for j in range(i + 1) if i == count - 1 or count == 2]


def mix_kernel(axes, sizes, count, scale_all, *refs):
    images = refs[:count]
    residuals = refs[count : 2 * count]
    prior = refs[2 * count]
    o_ref, gram_ref, out_ref, slots0, slots1, held0, held1, s0, r0, s1, r1 = refs[2 * count + 1 :]
    slots, held, send_sems, recv_sems = (slots0, slots1), (held0, held1), (s0, s1), (r0, r1)
    barrier = pltpu.get_barrier_semaphore()
    peers = []
    for axis, n in zip(axes, sizes):
        me = lax.axis_index(axis)
        peers.append([lax.rem(me + d, n) for d in range(1, n)])
        for peer in peers[-1]:
            pl.semaphore_signal(barrier, inc=1, device_id={axis: peer}, device_id_type=MESH)
    rows, width = images[0].shape
    wanted = new_products(count)

    def block(at, sums):
        columns = pl.ds(pl.multiple_of(at * 128, 128), 128)
        return tuple(
            total + jnp.sum((residuals[i][:, columns] * residuals[j][:, columns]).reshape(rows // 8, 8, 128), axis=0)
            for (i, j), total in zip(wanted, sums)
        )

    zero = jnp.zeros((8, 128), jnp.float32)
    sums = lax.fori_loop(0, width // 128, block, (zero,) * len(wanted), unroll=4)
    pl.semaphore_wait(barrier, sum(sizes) - len(sizes))
    local = jnp.concatenate(sums, axis=0)
    for stage, axis in enumerate(axes):
        held[stage][...] = local
        copies = [
            send(held[stage], slots[stage].at[d], send_sems[stage].at[d], recv_sems[stage].at[d], axis, peer)
            for d, peer in enumerate(peers[stage])
        ]
        for d, copy in enumerate(copies):
            copy.wait()
            local = local + slots[stage][d]
    gram = [[None] * count for _ in range(count)]
    for i in range(count):
        for j in range(i + 1):
            if (i, j) in wanted:
                at = 8 * wanted.index((i, j))
                value = jnp.broadcast_to(jnp.sum(local[at : at + 8], keepdims=True), (8, 128))
            else:
                value = prior[ITERS * i + j]
            gram[i][j] = gram[j][i] = value
    for i in range(ITERS):
        for j in range(ITERS):
            if i < count and j <= i:
                gram_ref[ITERS * i + j] = gram[i][j]
            else:
                gram_ref[ITERS * i + j] = zero
    system = [
        [gram[i][j] / scale_all + (LAMBDA if i == j else 0.0) for j in range(count)] for i in range(count)
    ]
    unscaled = solve_values(system, [jnp.ones((8, 128), jnp.float32)] * count)
    whole = unscaled[0]
    for value in unscaled[1:]:
        whole = whole + value
    weights = [value / whole for value in unscaled]
    for j in range(count):
        out_ref[j] = weights[j]
    tiles = [jnp.broadcast_to(weight[:1], (rows, 128)) for weight in weights]

    def combine(at, carry):
        columns = pl.ds(pl.multiple_of(at * 128, 128), 128)
        total = tiles[0] * images[0][:, columns]
        for j in range(1, count):
            total = total + tiles[j] * images[j][:, columns]
        o_ref[:, columns] = total
        return carry

    lax.fori_loop(0, width // 128, combine, 0, unroll=4)


def mix(images, residuals, prior, axes, scale_all, collective_id):
    sizes = tuple(lax.axis_size(axis) for axis in axes)
    count = len(images)
    current, gram, _ = pl.pallas_call(
        functools.partial(mix_kernel, axes, sizes, count, scale_all),
        out_shape=[
            jax.ShapeDtypeStruct(images[0].shape, jnp.float32),
            jax.ShapeDtypeStruct((ITERS * ITERS, 8, 128), jnp.float32),
            jax.ShapeDtypeStruct((count, 8, 128), jnp.float32),
        ],
        in_specs=[VMEM] * (2 * count + 1),
        out_specs=[VMEM] * 3,
        scratch_shapes=[pltpu.VMEM((n, 8 * len(new_products(count)), 128), jnp.float32) for n in sizes]
        + [pltpu.VMEM((8 * len(new_products(count)), 128), jnp.float32)] * len(sizes)
        + [pltpu.SemaphoreType.DMA((n,)) for n in sizes for _ in range(2)],
        compiler_params=pltpu.CompilerParams(collective_id=collective_id, has_side_effects=True),
    )(*images, *residuals, prior)
    return current, gram


def on_device(injection, warm_start, gain_in, gain_out, w_query, w_key, w_value, w_out):
    seq_at = lax.axis_index("seq")
    feat = lax.axis_size("feat")
    seq = lax.axis_size("seq")
    tok_dev = injection.shape[0]
    width = gain_in.shape[0]
    head_cols = w_query.shape[1]
    kv_cols = w_key.shape[1]
    kv_local = kv_cols // HEAD_DIM
    group = HEADS // KV_HEADS
    rows = tok_dev // feat
    part = width // feat
    scale_all = float(tok_dev * seq * width)
    score_scale = 1.0 / math.sqrt(HEAD_DIM)
    w_kv = jnp.concatenate([w_key, w_value], axis=1)
    query_pos = seq_at * tok_dev + jnp.arange(tok_dev, dtype=jnp.int32)
    key_pos = jnp.arange(tok_dev * seq, dtype=jnp.int32)
    allowed = (query_pos[:, None] >= key_pos[None, :])[:, None, :]
    start = jnp.stack([injection.reshape(feat, rows, part), warm_start.reshape(feat, rows, part)], axis=1)
    start = exchange(start, "feat", 0).transpose(1, 2, 0, 3).reshape(2, rows, width).astype(jnp.float32)
    injection_full, current = start[0], start[1]
    evaluated = []
    residuals = []
    gram = None
    for iteration in range(ITERS):
        mixed = current + injection_full
        normed = (
            mixed * lax.rsqrt(jnp.mean(mixed * mixed, axis=1, keepdims=True) + EPS) * gain_in
        ).astype(jnp.bfloat16)
        tokens = gather(normed, "feat", 2, 1).reshape(tok_dev, width)
        key_value = jnp.dot(tokens, w_kv, preferred_element_type=jnp.float32).astype(jnp.bfloat16)
        queries = jnp.dot(tokens, w_query, preferred_element_type=jnp.float32).astype(jnp.bfloat16)
        pieces = gather(key_value, "seq", 1, 2).reshape(seq * tok_dev, 2 * kv_cols)
        heads = []
        for e in range(kv_local):
            key_head = pieces[:, e * HEAD_DIM : (e + 1) * HEAD_DIM]
            value_head = pieces[:, kv_cols + e * HEAD_DIM : kv_cols + (e + 1) * HEAD_DIM]
            query_head = queries[:, e * group * HEAD_DIM : (e + 1) * group * HEAD_DIM].reshape(
                tok_dev, group, HEAD_DIM
            )
            scores = (
                jnp.einsum("tgd,sd->tgs", query_head, key_head, preferred_element_type=jnp.float32)
                * score_scale
            )
            scores = jnp.where(allowed, scores, -1e30)
            weights = jnp.where(allowed, jnp.exp(scores - jnp.max(scores, axis=2, keepdims=True)), 0.0)
            row_sum = jnp.sum(weights, axis=2, keepdims=True)
            summed = jnp.einsum(
                "tgs,sd->tgd", weights.astype(jnp.bfloat16), value_head, preferred_element_type=jnp.float32
            )
            heads.append((summed / row_sum).astype(jnp.bfloat16).reshape(tok_dev, group * HEAD_DIM))
        attended = jnp.concatenate(heads, axis=1)
        partial = jnp.dot(attended, w_out, preferred_element_type=jnp.float32).astype(jnp.bfloat16)
        update = scatter(partial.reshape(feat, rows, width), "feat", 2, 3)
        summed = mixed + update
        image = (
            summed * lax.rsqrt(jnp.mean(summed * summed, axis=1, keepdims=True) + EPS) * gain_out
        )
        evaluated.append(image)
        residuals.append(image - current)
        if iteration == 0:
            current = image
            gram = jnp.zeros((ITERS * ITERS, 8, 128), jnp.float32)
        else:
            current, gram = mix(evaluated, residuals, gram, ("feat", "seq"), scale_all, 4 + iteration)
    final = current.reshape(rows, feat, part).transpose(1, 0, 2)
    return exchange(final, "feat", 4).reshape(tok_dev, part)


def solution(mesh):
    in_specs = (
        P("seq", "feat"),
        P("seq", "feat"),
        P(),
        P(),
        P(None, "feat"),
        P(None, "feat"),
        P(None, "feat"),
        P("feat", None),
    )
    out_specs = P("seq", "feat")
    return jax.shard_map(
        on_device, mesh=mesh, in_specs=in_specs, out_specs=out_specs, check_vma=False
    )
```

```python
import functools
import math

import jax
import jax.numpy as jnp
from jax import lax
from jax.experimental import pallas as pl
from jax.experimental.pallas import tpu as pltpu
from jax.sharding import PartitionSpec as P

HEADS = 40
KV_HEADS = 8
HEAD_DIM = 128
ITERS = 4

EPS = 1e-06
LAMBDA = 0.03
MESH = pl.DeviceIdType.MESH
VMEM = pl.BlockSpec(memory_space=pltpu.VMEM)


def greet(axis, peers):
    barrier = pltpu.get_barrier_semaphore()
    for peer in peers:
        pl.semaphore_signal(barrier, inc=1, device_id={axis: peer}, device_id_type=MESH)
    return barrier


def send(src, dst, send_sem, recv_sem, axis, target):
    copy = pltpu.make_async_remote_copy(
        src_ref=src, dst_ref=dst, send_sem=send_sem, recv_sem=recv_sem,
        device_id={axis: target}, device_id_type=MESH,
    )
    copy.start()
    return copy


def place(axis, n):
    me = lax.axis_index(axis)
    side = lax.rem(me, 2)
    mine = lax.div(me, 2)
    return me, side, mine, me + 1 - 2 * side, n // 2


def front_kernel(n, m, chunks, x_ref, w_kv, w_query, q_ref, o_ref, tok, kv_here, q_here,
                 feat_s, feat_r, up_s, up_r, side_s, side_r, load_sem):
    me, side, mine, partner, lines = place("feat", n)
    at_seq, row_side, level, row_partner, levels = place("seq", m)
    rows = x_ref.shape[0] // chunks
    tok_dev = o_ref.shape[1]
    span = tok_dev // chunks
    loads = [
        pltpu.make_async_copy(w_kv, kv_here, load_sem.at[0]),
        pltpu.make_async_copy(w_query, q_here, load_sem.at[1]),
        pltpu.make_async_copy(x_ref, tok.at[me], load_sem.at[2]),
    ]
    for load in loads:
        load.start()
    peers = [2 * lax.rem(mine + d, lines) + side for d in range(1, lines)]
    barrier = greet("feat", [partner] + peers)

    def hail(target):
        pl.semaphore_signal(barrier, inc=1, device_id={"seq": target}, device_id_type=MESH)

    @pl.when(level > 0)
    def _():
        hail(at_seq - 2)
        hail(row_partner)

    @pl.when(level == 0)
    def _():
        @pl.when(row_side == 1)
        def _():
            hail(row_partner)

    raised = lax.div(level + levels - 1, levels)
    goes_up = 1 - lax.div(level, levels - 1)
    goes_across = 1 - row_side * (1 - raised)
    pl.semaphore_wait(barrier, lines + goes_up + goes_across)

    pending = []
    arrivals = []
    for c in range(chunks):
        part = pl.ds(c * rows, rows)
        for d in range(1, lines):
            copy = send(x_ref.at[part], tok.at[me, part], feat_s.at[c, d], feat_r.at[c, d], "feat", peers[d - 1])
            arrivals.append((c, d, copy))
    for c in range(chunks):
        part = pl.ds(c * rows, rows)
        pending.append(
            send(x_ref.at[part], tok.at[me, part], feat_s.at[c, 0], feat_r.at[c, 0], "feat", partner)
        )
    for slot in range(m):
        @pl.when(slot > at_seq)
        def _():
            o_ref[slot] = jnp.zeros(o_ref.shape[1:], o_ref.dtype)

    for c, d, copy in arrivals:
        copy.wait_recv()
        part = pl.ds(c * rows, rows)
        here = tok.at[2 * lax.rem(mine - d + lines, lines) + side, part]
        at = lines - 1 + d
        pending.append(send(here, here, feat_s.at[c, at], feat_r.at[c, at], "feat", partner))
    for c, d, copy in arrivals:
        copy.wait_send()
    for copy in pending:
        copy.wait()
    for load in loads:
        load.wait()

    tile = 256
    width = tok.shape[-1]

    def project(weights, put, first, last):
        @pl.loop(first, last)
        def _(at):
            columns = pl.ds(pl.multiple_of(at * tile, tile), tile)
            put(
                columns,
                jnp.dot(
                    tok[...].reshape(tok_dev, width), weights[:, columns], preferred_element_type=jnp.float32
                ).astype(jnp.bfloat16),
            )

    def put_kv(columns, value):
        o_ref[at_seq, :, columns] = value

    def put_q(columns, value):
        q_ref[:, columns] = value

    project(kv_here, put_kv, 0, kv_here.shape[1] // tile)

    def step(c, k, axis_kind):
        here = o_ref.at[2 * (level - k) + row_side, pl.ds(c * span, span)]
        sems = (up_s, up_r) if axis_kind == "up" else (side_s, side_r)
        return pltpu.make_async_remote_copy(
            src_ref=here, dst_ref=here, send_sem=sems[0].at[c, k], recv_sem=sems[1].at[c, k],
            device_id={"seq": at_seq + 2 if axis_kind == "up" else row_partner}, device_id_type=MESH,
        )

    def arrived(c, k):
        here = o_ref.at[2 * (level - k) + row_side, pl.ds(c * span, span)]
        return pltpu.make_async_remote_copy(
            src_ref=here, dst_ref=here, send_sem=up_s.at[c, k - 1], recv_sem=up_r.at[c, k - 1],
            device_id={"seq": at_seq - 2}, device_id_type=MESH,
        )

    def crossed(c, k):
        here = o_ref.at[2 * (level - k) + 1 - row_side, pl.ds(c * span, span)]
        return pltpu.make_async_remote_copy(
            src_ref=here, dst_ref=here, send_sem=side_s.at[c, k], recv_sem=side_r.at[c, k],
            device_id={"seq": row_partner}, device_id_type=MESH,
        )

    for c in range(chunks):
        @pl.when(level + 1 < levels)
        def _():
            step(c, 0, "up").start()

        @pl.when(row_side == 0)
        def _():
            step(c, 0, "side").start()

    tiles = q_here.shape[1] // tile
    for k in range(1, levels):
        if k == 1:
            project(q_here, put_q, 0, tiles - tiles // 2)
        if k == 2:
            project(q_here, put_q, tiles - tiles // 2, tiles)

        @pl.when(level >= k)
        def _():
            for c in range(chunks):
                arrived(c, k).wait_recv()

                @pl.when(level + 1 < levels)
                def _():
                    step(c, k, "up").start()

                step(c, k, "side").start()

    for k in range(levels):
        for c in range(chunks):
            @pl.when(level >= k)
            def _():
                @pl.when(level + 1 < levels)
                def _():
                    step(c, k, "up").wait_send()

                if k > 0:
                    step(c, k, "side").wait_send()
                    crossed(c, k).wait_recv()
                else:
                    @pl.when(row_side == 0)
                    def _():
                        step(c, 0, "side").wait_send()

                    @pl.when(row_side == 1)
                    def _():
                        crossed(c, 0).wait_recv()


def front(x, w_kv, w_query, chunks, collective_id):
    n, m = lax.axis_size("feat"), lax.axis_size("seq")
    tok_dev = n * x.shape[0]
    dma = pltpu.SemaphoreType.DMA
    anywhere = pl.BlockSpec(memory_space=pl.ANY)
    return pl.pallas_call(
        functools.partial(front_kernel, n, m, chunks),
        out_shape=[
            jax.ShapeDtypeStruct((tok_dev, w_query.shape[1]), x.dtype),
            jax.ShapeDtypeStruct((m, tok_dev, w_kv.shape[1]), x.dtype),
        ],
        in_specs=[VMEM, anywhere, anywhere],
        out_specs=[VMEM, VMEM],
        scratch_shapes=[
            pltpu.VMEM((n,) + x.shape, x.dtype),
            pltpu.VMEM(w_kv.shape, w_kv.dtype),
            pltpu.VMEM(w_query.shape, w_query.dtype),
            dma((chunks, n)), dma((chunks, n)),
            dma((chunks, m // 2)), dma((chunks, m // 2)),
            dma((chunks, m // 2)), dma((chunks, m // 2)),
            dma((3,)),
        ],
        compiler_params=pltpu.CompilerParams(collective_id=collective_id, has_side_effects=True),
    )(x, w_kv, w_query)


def scatter_kernel(n, chunks, a_ref, w_ref, o_ref, w_here, parts, near, outgoing, far,
                   near_s, near_r, far_s, far_r, load_sem):
    me, side, mine, partner, lines = place("feat", n)
    rows, width = o_ref.shape
    span = width // chunks
    tile = 256
    lined = [lax.rem(mine + d, lines) for d in range(lines)]
    loads = []
    for c in range(chunks):
        part = pl.ds(c * span, span)
        loads.append(pltpu.make_async_copy(w_ref.at[:, part], w_here.at[:, part], load_sem.at[c]))
        loads[-1].start()
    barrier = greet("feat", [partner] + [2 * line + side for line in lined[1:]])
    nears = {}
    fars = {}

    def pass_on(c):
        part = pl.ds(c * span, span)
        for d in range(1, lines):
            nears[c, d].wait_recv()
            outgoing[d, :, part] = (
                parts[2 * lined[d] + side, :, part].astype(jnp.float32) + near[d, :, part].astype(jnp.float32)
            ).astype(jnp.bfloat16)
            fars[c, d] = send(
                outgoing.at[d, :, part], far.at[d, :, part], far_s.at[c, d], far_r.at[c, d], "feat",
                2 * lined[d] + side,
            )

    def finish(c):
        part = pl.ds(c * span, span)
        nears[c, 0].wait_recv()
        total = parts[me, :, part].astype(jnp.float32) + near[0, :, part].astype(jnp.float32)
        for d in range(1, lines):
            fars[c, d].wait_recv()
            total = total + far[d, :, part].astype(jnp.float32)
        o_ref[:, part] = total

    for c in range(chunks):
        loads[c].wait()

        @pl.loop(c * (span // tile), (c + 1) * (span // tile))
        def _(at):
            columns = pl.ds(pl.multiple_of(at * tile, tile), tile)
            parts[:, :, columns] = (
                jnp.dot(a_ref[...], w_here[:, columns], preferred_element_type=jnp.float32)
                .astype(jnp.bfloat16)
                .reshape(n, rows, tile)
            )

        if c == 0:
            pl.semaphore_wait(barrier, lines)
        part = pl.ds(c * span, span)
        for d in list(range(1, lines)) + [0]:
            nears[c, d] = send(
                parts.at[2 * lined[d] + 1 - side, :, part], near.at[d, :, part],
                near_s.at[c, d], near_r.at[c, d], "feat", partner,
            )
        if c > 0:
            pass_on(c - 1)
    pass_on(chunks - 1)
    for c in range(chunks):
        finish(c)
    for copy in list(nears.values()) + list(fars.values()):
        copy.wait_send()


def scatter(attended, w_out, chunks, collective_id):
    n = lax.axis_size("feat")
    lines = n // 2
    rows, width = attended.shape[0] // n, w_out.shape[1]
    buffer = pltpu.VMEM((lines, rows, width), attended.dtype)
    dma = pltpu.SemaphoreType.DMA
    return pl.pallas_call(
        functools.partial(scatter_kernel, n, chunks),
        out_shape=jax.ShapeDtypeStruct((rows, width), jnp.float32),
        in_specs=[VMEM, pl.BlockSpec(memory_space=pl.ANY)],
        out_specs=VMEM,
        scratch_shapes=[
            pltpu.VMEM(w_out.shape, w_out.dtype), pltpu.VMEM((n, rows, width), attended.dtype)
        ]
        + [buffer] * 3 + [dma((chunks, lines))] * 4 + [dma((chunks,))],
        compiler_params=pltpu.CompilerParams(collective_id=collective_id, has_side_effects=True),
    )(attended, w_out)


def exchange_kernel(axis, n, x_ref, o_ref, send_sem, recv_sem, own_sem):
    me = lax.axis_index(axis)
    peers = [lax.rem(me + d, n) for d in range(1, n)]
    barrier = greet(axis, peers)
    own = pltpu.make_async_copy(x_ref.at[me], o_ref.at[me], own_sem)
    own.start()
    pl.semaphore_wait(barrier, n - 1)
    copies = [
        send(x_ref.at[peer], o_ref.at[me], send_sem.at[d], recv_sem.at[d], axis, peer)
        for d, peer in enumerate(peers)
    ]
    for copy in copies:
        copy.wait()
    own.wait()


def exchange(x, axis, collective_id):
    n = lax.axis_size(axis)
    return pl.pallas_call(
        functools.partial(exchange_kernel, axis, n),
        out_shape=jax.ShapeDtypeStruct(x.shape, x.dtype),
        in_specs=[VMEM],
        out_specs=VMEM,
        scratch_shapes=[
            pltpu.SemaphoreType.DMA((n,)),
            pltpu.SemaphoreType.DMA((n,)),
            pltpu.SemaphoreType.DMA,
        ],
        compiler_params=pltpu.CompilerParams(collective_id=collective_id, has_side_effects=True),
    )(x)


def solve_values(rows, values):
    size = len(values)
    rows = [list(row) for row in rows]
    values = list(values)
    for pivot in range(size):
        for below in range(pivot + 1, size):
            ratio = rows[below][pivot] / rows[pivot][pivot]
            for at in range(pivot, size):
                rows[below][at] = rows[below][at] - ratio * rows[pivot][at]
            values[below] = values[below] - ratio * values[pivot]
    result = [None] * size
    for pivot in reversed(range(size)):
        running = values[pivot]
        for later in range(pivot + 1, size):
            running = running - rows[pivot][later] * result[later]
        result[pivot] = running / rows[pivot][pivot]
    return result


def new_products(count):
    return [(i, j) for i in range(count) for j in range(i + 1) if i == count - 1 or count == 2]


def mix_kernel(axes, sizes, count, scale_all, *refs):
    images = refs[:count]
    residuals = refs[count : 2 * count]
    prior = refs[2 * count]
    o_ref, gram_ref, out_ref, slots0, slots1, held0, held1, s0, r0, s1, r1 = refs[2 * count + 1 :]
    slots, held, send_sems, recv_sems = (slots0, slots1), (held0, held1), (s0, s1), (r0, r1)
    barrier = pltpu.get_barrier_semaphore()
    peers = []
    for axis, n in zip(axes, sizes):
        me = lax.axis_index(axis)
        peers.append([lax.rem(me + d, n) for d in range(1, n)])
        for peer in peers[-1]:
            pl.semaphore_signal(barrier, inc=1, device_id={axis: peer}, device_id_type=MESH)
    rows, width = images[0].shape
    wanted = new_products(count)

    def block(at, sums):
        columns = pl.ds(pl.multiple_of(at * 128, 128), 128)
        return tuple(
            total + jnp.sum((residuals[i][:, columns] * residuals[j][:, columns]).reshape(rows // 8, 8, 128), axis=0)
            for (i, j), total in zip(wanted, sums)
        )

    zero = jnp.zeros((8, 128), jnp.float32)
    sums = lax.fori_loop(0, width // 128, block, (zero,) * len(wanted), unroll=4)
    pl.semaphore_wait(barrier, sum(sizes) - len(sizes))
    local = jnp.concatenate(sums, axis=0)
    for stage, axis in enumerate(axes):
        held[stage][...] = local
        copies = [
            send(held[stage], slots[stage].at[d], send_sems[stage].at[d], recv_sems[stage].at[d], axis, peer)
            for d, peer in enumerate(peers[stage])
        ]
        for d, copy in enumerate(copies):
            copy.wait()
            local = local + slots[stage][d]
    gram = [[None] * count for _ in range(count)]
    for i in range(count):
        for j in range(i + 1):
            if (i, j) in wanted:
                at = 8 * wanted.index((i, j))
                value = jnp.broadcast_to(jnp.sum(local[at : at + 8], keepdims=True), (8, 128))
            else:
                value = prior[ITERS * i + j]
            gram[i][j] = gram[j][i] = value
    for i in range(ITERS):
        for j in range(ITERS):
            if i < count and j <= i:
                gram_ref[ITERS * i + j] = gram[i][j]
            else:
                gram_ref[ITERS * i + j] = zero
    system = [
        [gram[i][j] / scale_all + (LAMBDA if i == j else 0.0) for j in range(count)] for i in range(count)
    ]
    unscaled = solve_values(system, [jnp.ones((8, 128), jnp.float32)] * count)
    whole = unscaled[0]
    for value in unscaled[1:]:
        whole = whole + value
    weights = [value / whole for value in unscaled]
    for j in range(count):
        out_ref[j] = weights[j]
    tiles = [jnp.broadcast_to(weight[:1], (rows, 128)) for weight in weights]

    def combine(at, carry):
        columns = pl.ds(pl.multiple_of(at * 128, 128), 128)
        total = tiles[0] * images[0][:, columns]
        for j in range(1, count):
            total = total + tiles[j] * images[j][:, columns]
        o_ref[:, columns] = total
        return carry

    lax.fori_loop(0, width // 128, combine, 0, unroll=4)


def mix(images, residuals, prior, axes, scale_all, collective_id):
    sizes = tuple(lax.axis_size(axis) for axis in axes)
    count = len(images)
    current, gram, _ = pl.pallas_call(
        functools.partial(mix_kernel, axes, sizes, count, scale_all),
        out_shape=[
            jax.ShapeDtypeStruct(images[0].shape, jnp.float32),
            jax.ShapeDtypeStruct((ITERS * ITERS, 8, 128), jnp.float32),
            jax.ShapeDtypeStruct((count, 8, 128), jnp.float32),
        ],
        in_specs=[VMEM] * (2 * count + 1),
        out_specs=[VMEM] * 3,
        scratch_shapes=[pltpu.VMEM((n, 8 * len(new_products(count)), 128), jnp.float32) for n in sizes]
        + [pltpu.VMEM((8 * len(new_products(count)), 128), jnp.float32)] * len(sizes)
        + [pltpu.SemaphoreType.DMA((n,)) for n in sizes for _ in range(2)],
        compiler_params=pltpu.CompilerParams(collective_id=collective_id, has_side_effects=True),
    )(*images, *residuals, prior)
    return current, gram


def on_device(injection, warm_start, gain_in, gain_out, w_query, w_key, w_value, w_out):
    seq_at = lax.axis_index("seq")
    feat = lax.axis_size("feat")
    seq = lax.axis_size("seq")
    tok_dev = injection.shape[0]
    width = gain_in.shape[0]
    head_cols = w_query.shape[1]
    kv_cols = w_key.shape[1]
    kv_local = kv_cols // HEAD_DIM
    group = HEADS // KV_HEADS
    rows = tok_dev // feat
    part = width // feat
    scale_all = float(tok_dev * seq * width)
    score_scale = 1.0 / math.sqrt(HEAD_DIM)
    w_kv = jnp.concatenate([w_key, w_value], axis=1)
    query_pos = seq_at * tok_dev + jnp.arange(tok_dev, dtype=jnp.int32)
    key_pos = jnp.arange(tok_dev * seq, dtype=jnp.int32)
    allowed = (query_pos[:, None] >= key_pos[None, :])[:, None, :]
    start = jnp.stack([injection.reshape(feat, rows, part), warm_start.reshape(feat, rows, part)], axis=1)
    start = exchange(start, "feat", 0).transpose(1, 2, 0, 3).reshape(2, rows, width).astype(jnp.float32)
    injection_full, current = start[0], start[1]
    evaluated = []
    residuals = []
    gram = None
    for iteration in range(ITERS):
        mixed = current + injection_full
        normed = (
            mixed * lax.rsqrt(jnp.mean(mixed * mixed, axis=1, keepdims=True) + EPS) * gain_in
        ).astype(jnp.bfloat16)
        queries, pieces = front(normed, w_kv, w_query, 2, 1)
        pieces = pieces.reshape(seq * tok_dev, 2 * kv_cols)
        heads = []
        for e in range(kv_local):
            key_head = pieces[:, e * HEAD_DIM : (e + 1) * HEAD_DIM]
            value_head = pieces[:, kv_cols + e * HEAD_DIM : kv_cols + (e + 1) * HEAD_DIM]
            query_head = queries[:, e * group * HEAD_DIM : (e + 1) * group * HEAD_DIM].reshape(
                tok_dev, group, HEAD_DIM
            )
            scores = (
                jnp.einsum("tgd,sd->tgs", query_head, key_head, preferred_element_type=jnp.float32)
                * score_scale
            )
            scores = jnp.where(allowed, scores, -1e30)
            weights = jnp.where(allowed, jnp.exp(scores - jnp.max(scores, axis=2, keepdims=True)), 0.0)
            row_sum = jnp.sum(weights, axis=2, keepdims=True)
            summed = jnp.einsum(
                "tgs,sd->tgd", weights.astype(jnp.bfloat16), value_head, preferred_element_type=jnp.float32
            )
            heads.append((summed / row_sum).astype(jnp.bfloat16).reshape(tok_dev, group * HEAD_DIM))
        attended = jnp.concatenate(heads, axis=1)
        update = scatter(attended, w_out, 5, 3)
        summed = mixed + update
        image = (
            summed * lax.rsqrt(jnp.mean(summed * summed, axis=1, keepdims=True) + EPS) * gain_out
        )
        evaluated.append(image)
        residuals.append(image - current)
        if iteration == 0:
            current = image
            gram = jnp.zeros((ITERS * ITERS, 8, 128), jnp.float32)
        else:
            current, gram = mix(evaluated, residuals, gram, ("feat", "seq"), scale_all, 4 + iteration)
    final = current.reshape(rows, feat, part).transpose(1, 0, 2)
    return exchange(final, "feat", 4).reshape(tok_dev, part)


def solution(mesh):
    in_specs = (
        P("seq", "feat"),
        P("seq", "feat"),
        P(),
        P(),
        P(None, "feat"),
        P(None, "feat"),
        P(None, "feat"),
        P("feat", None),
    )
    out_specs = P("seq", "feat")
    return jax.shard_map(
        on_device, mesh=mesh, in_specs=in_specs, out_specs=out_specs, check_vma=False
    )
```
